256 devices in a mesh: seq: 8 (over y, x_lo), blk: 32 (over z, x_hi, core).
Axes of the slice: x: 4 (x_hi: 2, x_lo: 2; x = x_hi * 2 + x_lo), y: 4, z: 8, core: 2. Of those that a mesh axis runs over, the one named last changes fastest.
Arguments:
- activations: bfloat16 [2, 64, 1024, 4096], P(None, 'blk', 'seq'), may hold values from -120 to 120, as said below
- out_grads: bfloat16 [2, 64, 1024, 4096], P(None, 'blk', 'seq'), may hold values from -120 to 120, as said below
- lengths: int32 [64], P('blk'), may hold values from 512 to 1024
- input_proj: bfloat16 [2, 64, 4096], replicated, may hold values from -0.09375 to 0.09375
- output_proj: bfloat16 [2, 64, 4096], replicated, may hold values from -0.09375 to 0.09375
- stored_proj: float32 [16384, 2, 64, 64], P(('seq', 'blk')), may hold values from -6 to 6
Outputs:
- scores: float32 [64, 16384], P('blk', 'seq')
The draws below stay inside these ranges and needn't reach their ends.
Inputs may be any that keep to these rules, and one draw needn't show every extreme that they name: `activations`: finite values. `out_grads`: finite values.
All inputs are finite; a program needn't handle non-finite values.
Results may differ from the reference program's by a relative error of at most 0.0003.
Values sent between devices are 32-bit elements; how exact they have to be, the bound alone decides.
No kernel may reach another device: no remote copies, remote signals or barrier semaphores. Data moves between devices by JAX's collectives and lax.ppermute only.
A program may use at most 64 MiB of HBM per device.

```python
import math
import jax
import jax.numpy as jnp
from jax import lax

D = 4096
R = 64
L = 2
ROLLOUTS = 64
SEQ = 1024
TRAIN = 16384


def shaped_draw(key, model_width):
    k_base, k_token = jax.random.split(key, 2)
    full_shape = (L, ROLLOUTS, SEQ, model_width)
    base_draw = jnp.clip(jax.random.normal(k_base, full_shape, jnp.float32), -4.0, 4.0)
    token_scale = jnp.exp(jax.random.uniform(k_token, (L, ROLLOUTS, SEQ, 1), jnp.float32, 0.0, math.log(10.0)))
    roll_place = jnp.arange(ROLLOUTS, dtype=jnp.float32) / max(ROLLOUTS - 1, 1)
    seq_place = jnp.arange(SEQ, dtype=jnp.float32) / max(SEQ - 1, 1)
    rise_factor = jnp.exp(0.5 * math.log(3.0) * (roll_place[:, None] + seq_place[None, :]))
    return (base_draw * token_scale * rise_factor[None, :, :, None]).astype(jnp.bfloat16)


def draw_activations(key, part):
    return shaped_draw(jax.random.fold_in(key, 101), D)


def draw_out_grads(key, part):
    return shaped_draw(jax.random.fold_in(key, 202), D)


def plant(values, stream_key, low, top_value):
    dims = values.shape
    spot = [jax.random.randint(jax.random.fold_in(stream_key, axis), (), 0, dims[axis]) for axis in range(len(dims))]
    values = values.at[tuple(spot)].set(low)
    longest = dims.index(max(dims))
    spot[longest] = (spot[longest] + 1) % dims[longest]
    return values.at[tuple(spot)].set(top_value)


def block_scale(key, shape, pieces, low, largest):
    factor_of = 1.0
    for position, blocks in pieces:
        draws = jax.random.uniform(jax.random.fold_in(jax.random.fold_in(key, 6), position), (blocks,), jnp.float32, low / len(pieces), largest / len(pieces))
        factor_of = factor_of * jnp.repeat(jnp.exp(draws), shape[position] // blocks).reshape((-1,) + (1,) * (len(shape) - 1 - position))
    return factor_of


def normal_values(key, dims, spread, reach, cuts=(), kind=jnp.bfloat16):
    array = spread * jax.random.normal(key, dims, jnp.float32)
    if cuts:
        array = array * block_scale(key, dims, cuts, -0.22, 0.18)
    return jnp.clip(array, -reach, reach).astype(kind)


def setup_inputs(seed: int = 0) -> dict:
    key_list = jax.random.split(jax.random.key(seed), 7)
    activations = draw_activations(jax.random.fold_in(key_list[6], 71), 0)
    out_grads = draw_out_grads(jax.random.fold_in(key_list[6], 71), 0)
    lengths = plant(jax.random.randint(key_list[2], (ROLLOUTS,), SEQ // 2, SEQ + 1), jax.random.fold_in(key_list[2], 1), SEQ // 2, SEQ).astype(jnp.int32)
    input_proj = normal_values(key_list[3], (L, R, D), D ** -0.5, 0.09375)
    output_proj = normal_values(key_list[4], (L, R, D), D ** -0.5, 0.09375)
    stored_proj = normal_values(key_list[5], (TRAIN, L, R, R), 1.0, 6.0, ((0, 256),), jnp.float32)
    return dict(activations=activations, out_grads=out_grads, lengths=lengths, input_proj=input_proj, output_proj=output_proj, stored_proj=stored_proj)


damping = 0.1

def damped_inverse(moment, token_count):
    moment_mean = moment / token_count
    proj_rank = moment_mean.shape[-1]
    identity = jnp.eye(proj_rank, dtype=jnp.float32)
    trace_part = jnp.trace(moment_mean, axis1=1, axis2=2)
    damped = moment_mean + (damping * trace_part / proj_rank)[:, None, None] * identity
    factor_low = jnp.linalg.cholesky(damped)
    return jax.vmap(lambda lower: jax.scipy.linalg.cho_solve((lower, True), identity))(factor_low)

def reference(activations, out_grads, lengths, input_proj, output_proj, stored_proj):
    hp = lax.Precision.HIGHEST
    positions = jnp.arange(SEQ, dtype=jnp.int32)
    live_mask = (positions[None, :] < lengths[:, None]).astype(jnp.float32)
    token_count = jnp.sum(live_mask)
    moments_in = []
    moments_out = []
    grad_layers = []
    for layer in range(L):

        def one_rollout(carry, item):
            tokens_in, tokens_out, mask_row = item
            projected_in = jnp.dot(tokens_in.astype(jnp.float32), input_proj[layer].T.astype(jnp.float32), preferred_element_type=jnp.float32) * mask_row[:, None]
            projected_out = jnp.dot(tokens_out.astype(jnp.float32), output_proj[layer].T.astype(jnp.float32), preferred_element_type=jnp.float32) * mask_row[:, None]
            sum_in, sum_out = carry
            sum_in = sum_in + jnp.dot(projected_in.T, projected_in, precision=hp)
            sum_out = sum_out + jnp.dot(projected_out.T, projected_out, precision=hp)
            return ((sum_in, sum_out), jnp.dot(projected_out.T, projected_in, precision=hp))
        zeros_rr = jnp.zeros((R, R), jnp.float32)
        (sum_in, sum_out), grad_proj = lax.scan(one_rollout, (zeros_rr, zeros_rr), (activations[layer], out_grads[layer], live_mask))
        moments_in.append(sum_in)
        moments_out.append(sum_out)
        grad_layers.append(grad_proj)
    factor_in = damped_inverse(jnp.stack(moments_in), token_count)
    factor_out = damped_inverse(jnp.stack(moments_out), token_count)
    grad_stack = jnp.stack(grad_layers)
    left_done = jnp.einsum('lap,lrpq->lraq', factor_out, grad_stack, precision=hp)
    precond = jnp.einsum('lraq,lqk->lrak', left_done, factor_in, precision=hp)
    scores = jnp.einsum('lrak,tlak->rt', precond, stored_proj, precision=hp)
    return scores / math.sqrt(L * R * R)
```

```python
import functools
import math

import jax
import jax.numpy as jnp
from jax import lax
from jax.experimental import pallas as pl
from jax.experimental.pallas import tpu as pltpu
from jax.sharding import Mesh, PartitionSpec as P


damping = 0.1
SEQ = ("y", "x_lo")
BLK = ("z", "x_hi", "core")
HALF = 64
WIDE = 128
f32 = jnp.float32
bf16 = jnp.bfloat16
NT = (((1,), (1,)), ((), ()))
NN = (((1,), (0,)), ((), ()))


def cost(flops, moved):
    return pl.CostEstimate(flops=flops, bytes_accessed=moved, transcendentals=0)


def lanes_of(shape):
    return lax.broadcasted_iota(jnp.int32, shape, len(shape) - 1)


def in_two(x):
    high = x.astype(bf16)
    return high, (x - high.astype(f32)).astype(bf16)


def three_pass(a, b, dims):
    dot = functools.partial(lax.dot_general, dimension_numbers=dims, preferred_element_type=f32)
    rows = a[0].shape[0]
    stacked = dot(jnp.concatenate(a, axis=0), b[0])
    return stacked[:rows] + (stacked[rows:] + dot(a[0], b[1]))


def project_kernel(length_ref, start_ref, act_hbm, grad_hbm, win_hbm, wout_hbm, out_ref, act, grad, win, wout, sems):
    layers, rolls, seq, width = act.shape
    cuts = sems.shape[2]
    depth = width // cuts
    sides = ((act_hbm, act, win_hbm, win), (grad_hbm, grad, wout_hbm, wout))

    def copies(l, side, k):
        big_from, big_to, weight_from, weight_to = sides[side]
        span = pl.ds(k * depth, depth)
        return (
            pltpu.make_async_copy(weight_from.at[l, :, span], weight_to.at[l, :, span], sems.at[l, side, k, 0]),
            pltpu.make_async_copy(
                big_from.at[l, :, :, span], big_to.at[l, :, :, span], sems.at[l, side, k, 1]
            ),
        )

    every = [(l, side, k) for l in range(layers) for k in range(cuts) for side in range(2)]
    for place in every:
        for copy in copies(*place):
            copy.start()
    dot = functools.partial(lax.dot_general, dimension_numbers=NT, preferred_element_type=f32)
    lane = lanes_of((HALF, WIDE))
    row = lax.broadcasted_iota(jnp.int32, (HALF, WIDE), 0)
    position = lax.broadcasted_iota(jnp.int32, (seq, WIDE), 0)
    part = HALF // out_ref.shape[0]
    for l in range(layers):
        halves = [None, None]
        for k in range(cuts):
            for side in range(2):
                for copy in copies(l, side, k):
                    copy.wait()
            span = slice(k * depth, (k + 1) * depth)
            for side in range(2):
                _, big, _, weight = sides[side]
                term = jnp.concatenate([dot(big[l, r, :, span], weight[l, :, span]) for r in range(rolls)], axis=0)
                halves[side] = term if k == 0 else halves[side] + term
        both = jnp.concatenate(halves, axis=1)
        grams = []
        count = jnp.int32(0)
        for r in range(rolls):
            live = length_ref[r] - start_ref[0]
            c = both[r * seq : (r + 1) * seq] * (position < live).astype(f32)
            grams.append(
                lax.dot_general(c.T, c, NN, precision=lax.Precision.HIGHEST, preferred_element_type=f32)
            )
            count += jnp.clip(live, 0, seq)
        pair = jnp.where(lane < HALF, grams[0][HALF:], pltpu.roll(grams[1][HALF:], HALF, 1))
        total = grams[0] + grams[1]
        moments = jnp.where(lane < HALF, total[:HALF], total[HALF:])
        moments = jnp.where((row == 0) & (lane == 1), count.astype(f32), moments)
        for y in range(out_ref.shape[0]):
            out_ref[y, l, 0:part] = pair[y * part : (y + 1) * part]
            out_ref[y, l, part : 2 * part] = moments[y * part : (y + 1) * part]


def project(lengths, start, activations, out_grads, input_proj, output_proj, parts):
    layers, rolls, seq, width = activations.shape
    rank = input_proj.shape[1]
    cuts = 4
    part = HALF // parts
    anywhere = pl.BlockSpec(memory_space=pl.ANY)
    return pl.pallas_call(
        project_kernel,
        in_specs=[pl.BlockSpec(memory_space=pltpu.SMEM)] * 2 + [anywhere] * 4,
        out_specs=pl.BlockSpec(memory_space=pltpu.VMEM),
        out_shape=jax.ShapeDtypeStruct((parts, layers, 2 * part, WIDE), f32),
        scratch_shapes=[
            pltpu.VMEM(activations.shape, activations.dtype),
            pltpu.VMEM(out_grads.shape, out_grads.dtype),
            pltpu.VMEM(input_proj.shape, input_proj.dtype),
            pltpu.VMEM(output_proj.shape, output_proj.dtype),
            pltpu.SemaphoreType.DMA((layers, 2, cuts, 2)),
        ],
        compiler_params=pltpu.CompilerParams(vmem_limit_bytes=67_043_328),
        cost_estimate=cost(4 * layers * rolls * seq * width * rank, 4 * layers * rolls * seq * width),
        name="project",
    )(lengths, start, activations, out_grads, input_proj, output_proj)


def pack_kernel(layer_ref, keep_top, keep_low, send_top, send_low, keep_ref, send_ref):
    for k in range(keep_ref.shape[0]):
        keep_ref[k] = jnp.concatenate([keep_top[:, 0, k, :], keep_low[:, 0, k, :]], axis=1)
        send_ref[k] = jnp.concatenate([send_top[:, 0, k, :], send_low[:, 0, k, :]], axis=1)


def pack(layer, stored):
    train, _, rank, _ = stored.shape
    chunk = 8
    steps = rank // 2 // chunk

    def spec(other, low):
        def at(i, layer):
            l = 1 - layer[0] if other else layer[0]
            return (0, l, i + (steps if low else 0), 0)

        return pl.BlockSpec((train, 1, chunk, rank), at)

    out = pl.BlockSpec((chunk, train, WIDE), lambda i, layer: (i, 0, 0))
    shape = jax.ShapeDtypeStruct((rank // 2, train, WIDE), f32)
    return pl.pallas_call(
        pack_kernel,
        grid_spec=pltpu.PrefetchScalarGridSpec(
            num_scalar_prefetch=1,
            grid=(steps,),
            in_specs=[spec(False, False), spec(False, True), spec(True, False), spec(True, True)],
            out_specs=[out, out],
        ),
        out_shape=[shape, shape],
        compiler_params=pltpu.CompilerParams(vmem_limit_bytes=12 * 2**20),
        cost_estimate=cost(10_000_000, 6 * 2**20),
        name="pack",
    )(layer, stored, stored, stored, stored)


def inverse_of_pair(a):
    step = 8
    lane = lanes_of((step, WIDE))
    sub = lax.broadcasted_iota(jnp.int32, (step, WIDE), 0)
    base = jnp.where(lane < HALF, 0, HALF)
    rows = [a[i * step : (i + 1) * step] for i in range(HALF // step)]

    def spread(x, m):
        return jnp.broadcast_to(x[m : m + 1], (step, WIDE))

    for block in range(HALF // step):
        first = block * step
        columns = [
            [jnp.take_along_axis(r, base + (first + j), axis=1) for j in range(step)] for r in rows
        ]
        inside = (lane - base >= first) & (lane - base < first + step)
        identity = jnp.where(lane - base == first + sub, 1.0, 0.0)
        panel = jnp.where(inside, identity, rows[block])
        diag = list(columns[block])
        for m in range(step):
            inverse = 1.0 / spread(diag[m], m)
            is_row = sub == m
            keep = jnp.where(is_row, 0.0, diag[m])
            for j in range(m + 1, step):
                scaled = spread(diag[j], m) * inverse
                diag[j] = jnp.where(is_row, scaled, diag[j] - keep * scaled)
            scaled = spread(panel, m) * inverse
            panel = jnp.where(is_row, scaled, panel - keep * scaled)
        spreads = [spread(panel, j) for j in range(step)]
        for i in range(HALF // step):
            if i == block:
                rows[i] = panel
                continue
            taken = [c * p for c, p in zip(columns[i], spreads)]
            while len(taken) > 1:
                taken = [x + y for x, y in zip(taken[::2], taken[1::2])]
            rows[i] = jnp.where(inside, 0.0, rows[i]) - taken[0]
    return jnp.concatenate(rows, axis=0)


def score_kernel(core_ref, got_ref, own, over, out_ref, rolled):
    parts = got_ref.shape[0] // 2
    part = HALF // parts
    blocks = 2 * (got_ref.shape[1] // part - 1)
    lane = lanes_of((HALF, WIDE))
    row = lax.broadcasted_iota(jnp.int32, (HALF, WIDE), 0)
    left = lane < HALF
    at = got_ref.shape[1] - part
    moments = jnp.concatenate([got_ref[2 * y, at:] + got_ref[2 * y + 1, at:] for y in range(parts)], axis=0)
    count = jnp.broadcast_to(moments[0:1, 1:2], (HALF, WIDE))
    moments = jnp.where((row == 0) & (lane == 1), jnp.broadcast_to(moments[1:2, 0:1], (HALF, WIDE)), moments)
    mean = moments / count
    diagonal = jnp.where((lane == row) | (lane == row + HALF), mean, 0.0)
    trace_in = jnp.sum(jnp.where(left, diagonal, 0.0))
    trace_out = jnp.sum(jnp.where(left, 0.0, diagonal))
    extra = jnp.where(left, trace_in, trace_out) * (damping / HALF)
    damped = mean + jnp.where((lane == row) | (lane == row + HALF), extra, 0.0)
    factors = inverse_of_pair(damped)
    top = jnp.where(left, factors, 0.0)
    right = jnp.concatenate([top, pltpu.roll(top, HALF, 1)], axis=0)
    empty = jnp.zeros_like(right)
    right = in_two(
        jnp.concatenate(
            [jnp.concatenate([right, empty], axis=1), jnp.concatenate([empty, right], axis=1)], axis=0
        )
    )
    outer = in_two(factors[:, HALF:])
    half_lane = lanes_of((HALF // 2, WIDE)) < HALF

    def block_of(i):
        z, x, core = i // 4, i // 2 % 2, i % 2
        at = (2 * z + core) * part
        return [got_ref[2 * y + x, at : at + part] for y in range(parts)]

    group = 16
    apart = HALF // 2 + 1
    for b in range(0, blocks, group):
        g = [
            jnp.concatenate(block_of(i), axis=0)
            for i in range(b, b + group)
        ]
        g = jnp.concatenate([jnp.concatenate(g[i : i + 2], axis=1) for i in range(0, group, 2)], axis=0)
        inner = three_pass(in_two(g), right, NN)
        inner = jnp.concatenate([inner[HALF * i : HALF * (i + 1)] for i in range(group // 2)], axis=1)
        done = three_pass(outer, in_two(inner), NN)
        for i in range(group):
            up = done[: HALF // 2, WIDE * i : WIDE * (i + 1)]
            low = done[HALF // 2 :, WIDE * i : WIDE * (i + 1)]
            at = 2 * (b + i)
            rolled[pl.ds(at * apart, HALF // 2)] = jnp.where(half_lane, up, pltpu.roll(low, HALF, 1))
            rolled[pl.ds((at + 1) * apart, HALF // 2)] = jnp.where(half_lane, pltpu.roll(up, HALF, 1), low)
    scores = jnp.zeros((2 * blocks, 2 * HALF), f32)
    deep = 8
    for k in range(0, HALF // 2, deep):
        first = jnp.concatenate([rolled[pl.ds(k + i, 2 * blocks, apart)] for i in range(deep)], axis=1)
        second = jnp.concatenate([jnp.concatenate([own[k + i], over[k + i]], axis=0) for i in range(deep)], axis=1)
        scores += three_pass(in_two(first), in_two(second), NT)
    scores *= 1.0 / math.sqrt(2 * HALF * HALF)
    out_ref[...] = jnp.where(core_ref[0] == 0, scores, pltpu.roll(scores, HALF, 1))


def score(place, got, own, over):
    blocks = 2 * (got.shape[1] // (2 * HALF // got.shape[0]) - 1)
    vmem = pl.BlockSpec(memory_space=pltpu.VMEM)
    return pl.pallas_call(
        score_kernel,
        in_specs=[pl.BlockSpec(memory_space=pltpu.SMEM)] + [vmem] * 3,
        out_specs=vmem,
        out_shape=jax.ShapeDtypeStruct((2 * blocks, WIDE), f32),
        scratch_shapes=[
            pltpu.VMEM((2 * blocks * (HALF // 2 + 1), WIDE), f32),
        ],
        compiler_params=pltpu.CompilerParams(vmem_limit_bytes=16 * 2**20),
        cost_estimate=cost(200_000_000, 6 * 2**20),
        name="score",
    )(place, got, own, over)


def shards(activations, out_grads, lengths, input_proj, output_proj, stored_proj):
    seq_count = lax.axis_size(SEQ)
    core = lax.axis_index("core")
    seq_dev = activations.shape[2]
    start = (lax.axis_index(SEQ) * seq_dev).astype(jnp.int32).reshape(1)
    place = core.astype(jnp.int32).reshape(1)
    terms = project(lengths, start, activations, out_grads, input_proj, output_proj, seq_count)
    part = terms.shape[2] // 2
    terms = terms.reshape(-1, 2 * part, WIDE)
    arrived = lax.all_to_all(terms, SEQ + ("core",), 0, 0, tiled=True)
    seq_sum = arrived.reshape(seq_count, 2, 2 * part, WIDE).sum(axis=0)
    moments = seq_sum[:, part:].sum(axis=0)
    rows = jnp.concatenate([seq_sum[:, :part].reshape(-1, WIDE), moments], axis=0)
    z_count = lax.axis_size("z")
    z_all = lax.all_to_all(jnp.broadcast_to(rows, (z_count, *rows.shape)), "z", 0, 0, tiled=True)
    moments = z_all[:, 2 * part :].sum(axis=0)
    rows = jnp.concatenate([z_all[:, : 2 * part].reshape(-1, WIDE), moments], axis=0)
    rest = SEQ + ("x_hi",)
    got = lax.all_to_all(jnp.broadcast_to(rows, (lax.axis_size(rest), *rows.shape)), rest, 0, 0, tiled=True)
    own, send = pack(place, stored_proj)
    over = lax.ppermute(send, "core", [(0, 1), (1, 0)])
    partial = score(place, got, own, over)
    back = lax.all_to_all(partial.reshape(-1, 2, WIDE), BLK, 0, 0, tiled=True)
    back = back.reshape(-1, 2, 2, WIDE).sum(axis=1)
    return jnp.swapaxes(back, 0, 1).reshape(2, -1)


def solution(mesh):
    seq, blk = mesh.shape["seq"], mesh.shape["blk"]
    fine = Mesh(mesh.devices.reshape(seq // 2, 2, blk // 4, 2, 2), SEQ + BLK)
    return jax.shard_map(
        shards,
        mesh=fine,
        in_specs=(
            P(None, BLK, SEQ, None),
            P(None, BLK, SEQ, None),
            P(BLK),
            P(),
            P(),
            P(SEQ + BLK, None, None, None),
        ),
        out_specs=P(BLK, SEQ),
        check_vma=False,
    )
```

```python
import functools
import math

import jax
import jax.numpy as jnp
from jax import lax
from jax.experimental import pallas as pl
from jax.experimental.pallas import tpu as pltpu
from jax.sharding import Mesh, PartitionSpec as P


damping = 0.1
SEQ = ("y", "x_lo")
BLK = ("z", "x_hi", "core")
HALF = 64
WIDE = 128
f32 = jnp.float32
bf16 = jnp.bfloat16
NT = (((1,), (1,)), ((), ()))
NN = (((1,), (0,)), ((), ()))


def cost(flops, moved):
    return pl.CostEstimate(flops=flops, bytes_accessed=moved, transcendentals=0)


def lanes_of(shape):
    return lax.broadcasted_iota(jnp.int32, shape, len(shape) - 1)


def in_two(x):
    high = x.astype(bf16)
    return high, (x - high.astype(f32)).astype(bf16)


def three_pass(a, b, dims):
    dot = functools.partial(lax.dot_general, dimension_numbers=dims, preferred_element_type=f32)
    rows = a[0].shape[0]
    stacked = dot(jnp.concatenate(a, axis=0), b[0])
    return stacked[:rows] + (stacked[rows:] + dot(a[0], b[1]))


def project_kernel(length_ref, start_ref, place_ref, act_hbm, grad_hbm, win_hbm, wout_hbm, out_ref, act, grad, win, wout, sems):
    layers, rolls, seq, width = act.shape
    cuts = sems.shape[2]
    depth = width // cuts
    sides = ((act_hbm, act, win_hbm, win), (grad_hbm, grad, wout_hbm, wout))

    def copies(l, side, k):
        big_from, big_to, weight_from, weight_to = sides[side]
        span = pl.ds(k * depth, depth)
        return (
            pltpu.make_async_copy(weight_from.at[l, :, span], weight_to.at[l, :, span], sems.at[l, side, k, 0]),
            pltpu.make_async_copy(
                big_from.at[l, :, :, span], big_to.at[l, :, :, span], sems.at[l, side, k, 1]
            ),
        )

    every = [(l, side, k) for l in range(layers) for k in range(cuts) for side in range(2)]
    for place in every:
        for copy in copies(*place):
            copy.start()
    dot = functools.partial(lax.dot_general, dimension_numbers=NT, preferred_element_type=f32)
    lane = lanes_of((HALF, WIDE))
    row = lax.broadcasted_iota(jnp.int32, (HALF, WIDE), 0)
    position = lax.broadcasted_iota(jnp.int32, (seq, WIDE), 0)
    part = HALF // out_ref.shape[0]
    for l in range(layers):
        halves = [None, None]
        for k in range(cuts):
            for side in range(2):
                for copy in copies(l, side, k):
                    copy.wait()
            span = slice(k * depth, (k + 1) * depth)
            for side in range(2):
                _, big, _, weight = sides[side]
                term = jnp.concatenate([dot(big[l, r, :, span], weight[l, :, span]) for r in range(rolls)], axis=0)
                halves[side] = term if k == 0 else halves[side] + term
        both = jnp.concatenate(halves, axis=1)
        grams = []
        count = jnp.int32(0)
        for r in range(rolls):
            live = length_ref[r] - start_ref[0]
            c = both[r * seq : (r + 1) * seq] * (position < live).astype(f32)
            grams.append(
                lax.dot_general(c.T, c, NN, precision=lax.Precision.HIGHEST, preferred_element_type=f32)
            )
            count += jnp.clip(live, 0, seq)
        pair = jnp.where(lane < HALF, grams[0][HALF:], pltpu.roll(grams[1][HALF:], HALF, 1))
        total = grams[0] + grams[1]
        moments = jnp.where(lane < HALF, total[:HALF], total[HALF:])
        moments = jnp.where((row == 0) & (lane == 1), count.astype(f32), moments)
        for y in range(out_ref.shape[0]):
            out_ref[y, l, 0:part] = pair[y * part : (y + 1) * part]
            out_ref[y, l, part : 2 * part] = moments[y * part : (y + 1) * part]


def project(lengths, start, place, activations, out_grads, input_proj, output_proj, parts):
    layers, rolls, seq, width = activations.shape
    rank = input_proj.shape[1]
    cuts = 4
    part = HALF // parts
    anywhere = pl.BlockSpec(memory_space=pl.ANY)
    return pl.pallas_call(
        project_kernel,
        in_specs=[pl.BlockSpec(memory_space=pltpu.SMEM)] * 3 + [anywhere] * 4,
        out_specs=pl.BlockSpec(memory_space=pltpu.VMEM),
        out_shape=jax.ShapeDtypeStruct((parts, layers, 2 * part, WIDE), f32),
        scratch_shapes=[
            pltpu.VMEM(activations.shape, activations.dtype),
            pltpu.VMEM(out_grads.shape, out_grads.dtype),
            pltpu.VMEM(input_proj.shape, input_proj.dtype),
            pltpu.VMEM(output_proj.shape, output_proj.dtype),
            pltpu.SemaphoreType.DMA((layers, 2, cuts, 2)),
        ],
        compiler_params=pltpu.CompilerParams(vmem_limit_bytes=65_700_000),
        cost_estimate=cost(4 * layers * rolls * seq * width * rank, 4 * layers * rolls * seq * width),
        name="project",
    )(lengths, start, place, activations, out_grads, input_proj, output_proj)


def pack_kernel(layer_ref, keep_top, keep_low, send_top, send_low, keep_ref, send_ref):
    for k in range(keep_ref.shape[0]):
        keep_ref[k] = jnp.concatenate([keep_top[:, 0, k, :], keep_low[:, 0, k, :]], axis=1)
        send_ref[k] = jnp.concatenate([send_top[:, 0, k, :], send_low[:, 0, k, :]], axis=1)


def pack(layer, stored):
    train, _, rank, _ = stored.shape
    chunk = 8
    steps = rank // 2 // chunk

    def spec(other, low):
        def at(i, layer):
            l = 1 - layer[0] if other else layer[0]
            return (0, l, i + (steps if low else 0), 0)

        return pl.BlockSpec((train, 1, chunk, rank), at)

    out = pl.BlockSpec((chunk, train, WIDE), lambda i, layer: (i, 0, 0))
    shape = jax.ShapeDtypeStruct((rank // 2, train, WIDE), f32)
    return pl.pallas_call(
        pack_kernel,
        grid_spec=pltpu.PrefetchScalarGridSpec(
            num_scalar_prefetch=1,
            grid=(steps,),
            in_specs=[spec(False, False), spec(False, True), spec(True, False), spec(True, True)],
            out_specs=[out, out],
        ),
        out_shape=[shape, shape],
        compiler_params=pltpu.CompilerParams(vmem_limit_bytes=12 * 2**20),
        cost_estimate=cost(10_000_000, 6 * 2**20),
        name="pack",
    )(layer, stored, stored, stored, stored)


def inverse_of_pair(a):
    step = 8
    lane = lanes_of((step, WIDE))
    sub = lax.broadcasted_iota(jnp.int32, (step, WIDE), 0)
    base = jnp.where(lane < HALF, 0, HALF)
    rows = [a[i * step : (i + 1) * step] for i in range(HALF // step)]

    def spread(x, m):
        return jnp.broadcast_to(x[m : m + 1], (step, WIDE))

    for block in range(HALF // step):
        first = block * step
        columns = [
            [jnp.take_along_axis(r, base + (first + j), axis=1) for j in range(step)] for r in rows
        ]
        inside = (lane - base >= first) & (lane - base < first + step)
        identity = jnp.where(lane - base == first + sub, 1.0, 0.0)
        panel = jnp.where(inside, identity, rows[block])
        diag = list(columns[block])
        for m in range(step):
            inverse = 1.0 / spread(diag[m], m)
            is_row = sub == m
            keep = jnp.where(is_row, 0.0, diag[m])
            for j in range(m + 1, step):
                scaled = spread(diag[j], m) * inverse
                diag[j] = jnp.where(is_row, scaled, diag[j] - keep * scaled)
            scaled = spread(panel, m) * inverse
            panel = jnp.where(is_row, scaled, panel - keep * scaled)
        spreads = [spread(panel, j) for j in range(step)]
        for i in range(HALF // step):
            if i == block:
                rows[i] = panel
                continue
            taken = [c * p for c, p in zip(columns[i], spreads)]
            while len(taken) > 1:
                taken = [x + y for x, y in zip(taken[::2], taken[1::2])]
            rows[i] = jnp.where(inside, 0.0, rows[i]) - taken[0]
    return jnp.concatenate(rows, axis=0)


def score_kernel(core_ref, got_ref, own, over, out_ref, rolled):
    parts = got_ref.shape[0] // 2
    part = HALF // parts
    blocks = 2 * (got_ref.shape[1] // part - 1)
    lane = lanes_of((HALF, WIDE))
    row = lax.broadcasted_iota(jnp.int32, (HALF, WIDE), 0)
    left = lane < HALF
    at = got_ref.shape[1] - part
    moments = jnp.concatenate([got_ref[2 * y, at:] + got_ref[2 * y + 1, at:] for y in range(parts)], axis=0)
    count = jnp.broadcast_to(moments[0:1, 1:2], (HALF, WIDE))
    moments = jnp.where((row == 0) & (lane == 1), jnp.broadcast_to(moments[1:2, 0:1], (HALF, WIDE)), moments)
    mean = moments / count
    diagonal = jnp.where((lane == row) | (lane == row + HALF), mean, 0.0)
    trace_in = jnp.sum(jnp.where(left, diagonal, 0.0))
    trace_out = jnp.sum(jnp.where(left, 0.0, diagonal))
    extra = jnp.where(left, trace_in, trace_out) * (damping / HALF)
    damped = mean + jnp.where((lane == row) | (lane == row + HALF), extra, 0.0)
    factors = inverse_of_pair(damped)
    top = jnp.where(left, factors, 0.0)
    right = jnp.concatenate([top, pltpu.roll(top, HALF, 1)], axis=0)
    empty = jnp.zeros_like(right)
    right = in_two(
        jnp.concatenate(
            [jnp.concatenate([right, empty], axis=1), jnp.concatenate([empty, right], axis=1)], axis=0
        )
    )
    outer = in_two(factors[:, HALF:])
    half_lane = lanes_of((HALF // 2, WIDE)) < HALF

    def block_of(i):
        z, x, core = i // 4, i // 2 % 2, i % 2
        at = (2 * z + core) * part
        return [got_ref[2 * y + x, at : at + part] for y in range(parts)]

    group = 16
    apart = HALF // 2 + 1
    for b in range(0, blocks, group):
        g = [
            jnp.concatenate(block_of(i), axis=0)
            for i in range(b, b + group)
        ]
        g = jnp.concatenate([jnp.concatenate(g[i : i + 2], axis=1) for i in range(0, group, 2)], axis=0)
        inner = three_pass(in_two(g), right, NN)
        inner = jnp.concatenate([inner[HALF * i : HALF * (i + 1)] for i in range(group // 2)], axis=1)
        done = three_pass(outer, in_two(inner), NN)
        for i in range(group):
            up = done[: HALF // 2, WIDE * i : WIDE * (i + 1)]
            low = done[HALF // 2 :, WIDE * i : WIDE * (i + 1)]
            at = 2 * (b + i)
            rolled[pl.ds(at * apart, HALF // 2)] = jnp.where(half_lane, up, pltpu.roll(low, HALF, 1))
            rolled[pl.ds((at + 1) * apart, HALF // 2)] = jnp.where(half_lane, pltpu.roll(up, HALF, 1), low)
    scores = jnp.zeros((2 * blocks, 2 * HALF), f32)
    deep = 8
    for k in range(0, HALF // 2, deep):
        first = jnp.concatenate([rolled[pl.ds(k + i, 2 * blocks, apart)] for i in range(deep)], axis=1)
        second = jnp.concatenate([jnp.concatenate([own[k + i], over[k + i]], axis=0) for i in range(deep)], axis=1)
        scores += three_pass(in_two(first), in_two(second), NT)
    scores *= 1.0 / math.sqrt(2 * HALF * HALF)
    out_ref[...] = jnp.where(core_ref[0] == 0, scores, pltpu.roll(scores, HALF, 1))


def score(place, got, own, over):
    blocks = 2 * (got.shape[1] // (2 * HALF // got.shape[0]) - 1)
    vmem = pl.BlockSpec(memory_space=pltpu.VMEM)
    return pl.pallas_call(
        score_kernel,
        in_specs=[pl.BlockSpec(memory_space=pltpu.SMEM)] + [vmem] * 3,
        out_specs=vmem,
        out_shape=jax.ShapeDtypeStruct((2 * blocks, WIDE), f32),
        scratch_shapes=[
            pltpu.VMEM((2 * blocks * (HALF // 2 + 1), WIDE), f32),
        ],
        compiler_params=pltpu.CompilerParams(vmem_limit_bytes=16 * 2**20),
        cost_estimate=cost(200_000_000, 6 * 2**20),
        name="score",
    )(place, got, own, over)


def shards(activations, out_grads, lengths, input_proj, output_proj, stored_proj):
    seq_count = lax.axis_size(SEQ)
    core = lax.axis_index("core")
    seq_dev = activations.shape[2]
    start = (lax.axis_index(SEQ) * seq_dev).astype(jnp.int32).reshape(1)
    place = core.astype(jnp.int32).reshape(1)
    terms = project(lengths, start, place, activations, out_grads, input_proj, output_proj, seq_count)
    part = terms.shape[2] // 2
    terms = terms.reshape(-1, 2 * part, WIDE)
    arrived = lax.all_to_all(terms, SEQ + ("core",), 0, 0, tiled=True)
    seq_sum = arrived.reshape(seq_count, 2, 2 * part, WIDE).sum(axis=0)
    moments = seq_sum[:, part:].sum(axis=0)
    rows = jnp.concatenate([seq_sum[:, :part].reshape(-1, WIDE), moments], axis=0)
    z_count = lax.axis_size("z")
    z_all = lax.all_to_all(jnp.broadcast_to(rows, (z_count, *rows.shape)), "z", 0, 0, tiled=True)
    moments = z_all[:, 2 * part :].sum(axis=0)
    rows = jnp.concatenate([z_all[:, : 2 * part].reshape(-1, WIDE), moments], axis=0)
    rest = SEQ + ("x_hi",)
    got = lax.all_to_all(jnp.broadcast_to(rows, (lax.axis_size(rest), *rows.shape)), rest, 0, 0, tiled=True)
    own, send = pack(place, stored_proj)
    over = lax.ppermute(send, "core", [(0, 1), (1, 0)])
    partial = score(place, got, own, over)
    back = lax.all_to_all(partial.reshape(-1, 2, WIDE), BLK, 0, 0, tiled=True)
    back = back.reshape(-1, 2, 2, WIDE).sum(axis=1)
    return jnp.swapaxes(back, 0, 1).reshape(2, -1)


def solution(mesh):
    seq, blk = mesh.shape["seq"], mesh.shape["blk"]
    fine = Mesh(mesh.devices.reshape(seq // 2, 2, blk // 4, 2, 2), SEQ + BLK)
    return jax.shard_map(
        shards,
        mesh=fine,
        in_specs=(
            P(None, BLK, SEQ, None),
            P(None, BLK, SEQ, None),
            P(BLK),
            P(),
            P(),
            P(SEQ + BLK, None, None, None),
        ),
        out_specs=P(BLK, SEQ),
        check_vma=False,
    )
```

```python
import functools
import math

import jax
import jax.numpy as jnp
from jax import lax
from jax.experimental import pallas as pl
from jax.experimental.pallas import tpu as pltpu
from jax.sharding import Mesh, PartitionSpec as P


damping = 0.1
SEQ = ("y", "x_lo")
BLK = ("z", "x_hi", "core")
HALF = 64
WIDE = 128
f32 = jnp.float32
bf16 = jnp.bfloat16
NT = (((1,), (1,)), ((), ()))
NN = (((1,), (0,)), ((), ()))


def cost(flops, moved):
    return pl.CostEstimate(flops=flops, bytes_accessed=moved, transcendentals=0)


def lanes_of(shape):
    return lax.broadcasted_iota(jnp.int32, shape, len(shape) - 1)


def in_two(x):
    high = x.astype(bf16)
    return high, (x - high.astype(f32)).astype(bf16)


def three_pass(a, b, dims):
    dot = functools.partial(lax.dot_general, dimension_numbers=dims, preferred_element_type=f32)
    rows = a[0].shape[0]
    stacked = dot(jnp.concatenate(a, axis=0), b[0])
    return stacked[:rows] + (stacked[rows:] + dot(a[0], b[1]))


def project_kernel(length_ref, start_ref, place_ref, act_hbm, grad_hbm, win_hbm, wout_hbm, out_ref, act, grad, win, wout, sems):
    layers, rolls, seq, width = act.shape
    cuts = sems.shape[2]
    depth = width // cuts
    sides = ((act_hbm, act, win_hbm, win), (grad_hbm, grad, wout_hbm, wout))

    def copies(l, side, k):
        big_from, big_to, weight_from, weight_to = sides[side]
        span = pl.ds(k * depth, depth)
        return (
            pltpu.make_async_copy(weight_from.at[l, :, span], weight_to.at[l, :, span], sems.at[l, side, k, 0]),
            pltpu.make_async_copy(
                big_from.at[l, :, :, span], big_to.at[l, :, :, span], sems.at[l, side, k, 1]
            ),
        )

    every = [(l, side, k) for l in range(layers) for k in range(cuts) for side in range(2)]
    for place in every:
        for copy in copies(*place):
            copy.start()
    dot = functools.partial(lax.dot_general, dimension_numbers=NT, preferred_element_type=f32)
    lane = lanes_of((HALF, WIDE))
    row = lax.broadcasted_iota(jnp.int32, (HALF, WIDE), 0)
    position = lax.broadcasted_iota(jnp.int32, (seq, WIDE), 0)
    part = HALF // out_ref.shape[0]
    for l in range(layers):
        halves = [None, None]
        for k in range(cuts):
            for side in range(2):
                for copy in copies(l, side, k):
                    copy.wait()
            span = slice(k * depth, (k + 1) * depth)
            for side in range(2):
                _, big, _, weight = sides[side]
                term = jnp.concatenate([dot(big[l, r, :, span], weight[l, :, span]) for r in range(rolls)], axis=0)
                halves[side] = term if k == 0 else halves[side] + term
        both = jnp.concatenate(halves, axis=1)
        grams = []
        count = jnp.int32(0)
        for r in range(rolls):
            live = length_ref[r] - start_ref[0]
            c = both[r * seq : (r + 1) * seq] * (position < live).astype(f32)
            grams.append(
                lax.dot_general(c.T, c, NN, precision=lax.Precision.HIGHEST, preferred_element_type=f32)
            )
            count += jnp.clip(live, 0, seq)
        pair = jnp.where(lane < HALF, grams[0][HALF:], pltpu.roll(grams[1][HALF:], HALF, 1))
        total = grams[0] + grams[1]
        moments = jnp.where(lane < HALF, total[:HALF], total[HALF:])
        moments = jnp.where((row == 0) & (lane == 1), count.astype(f32), moments)
        for y in range(out_ref.shape[0]):
            out_ref[y, l, 0:part] = pair[y * part : (y + 1) * part]
            out_ref[y, l, part : 2 * part] = moments[y * part : (y + 1) * part]


def project(lengths, start, place, activations, out_grads, input_proj, output_proj, parts):
    layers, rolls, seq, width = activations.shape
    rank = input_proj.shape[1]
    cuts = 4
    part = HALF // parts
    anywhere = pl.BlockSpec(memory_space=pl.ANY)
    return pl.pallas_call(
        project_kernel,
        in_specs=[pl.BlockSpec(memory_space=pltpu.SMEM)] * 3 + [anywhere] * 4,
        out_specs=pl.BlockSpec(memory_space=pltpu.VMEM),
        out_shape=jax.ShapeDtypeStruct((parts, layers, 2 * part, WIDE), f32),
        scratch_shapes=[
            pltpu.VMEM(activations.shape, activations.dtype),
            pltpu.VMEM(out_grads.shape, out_grads.dtype),
            pltpu.VMEM(input_proj.shape, input_proj.dtype),
            pltpu.VMEM(output_proj.shape, output_proj.dtype),
            pltpu.SemaphoreType.DMA((layers, 2, cuts, 2)),
        ],
        compiler_params=pltpu.CompilerParams(vmem_limit_bytes=65_700_000),
        cost_estimate=cost(4 * layers * rolls * seq * width * rank, 4 * layers * rolls * seq * width),
        name="project",
    )(lengths, start, place, activations, out_grads, input_proj, output_proj)


def pack_kernel(layer_ref, keep_top, keep_low, send_top, send_low, keep_ref, send_ref):
    for k in range(keep_ref.shape[0]):
        keep_ref[k] = jnp.concatenate([keep_top[:, 0, k, :], keep_low[:, 0, k, :]], axis=1)
        send_ref[k] = jnp.concatenate([send_top[:, 0, k, :], send_low[:, 0, k, :]], axis=1)


def pack(layer, stored):
    train, _, rank, _ = stored.shape
    chunk = 8
    steps = rank // 2 // chunk

    def spec(other, low):
        def at(i, layer):
            l = 1 - layer[0] if other else layer[0]
            return (0, l, i + (steps if low else 0), 0)

        return pl.BlockSpec((train, 1, chunk, rank), at)

    out = pl.BlockSpec((chunk, train, WIDE), lambda i, layer: (i, 0, 0))
    shape = jax.ShapeDtypeStruct((rank // 2, train, WIDE), f32)
    return pl.pallas_call(
        pack_kernel,
        grid_spec=pltpu.PrefetchScalarGridSpec(
            num_scalar_prefetch=1,
            grid=(steps,),
            in_specs=[spec(False, False), spec(False, True), spec(True, False), spec(True, True)],
            out_specs=[out, out],
        ),
        out_shape=[shape, shape],
        compiler_params=pltpu.CompilerParams(vmem_limit_bytes=12 * 2**20),
        cost_estimate=cost(10_000_000, 6 * 2**20),
        name="pack",
    )(layer, stored, stored, stored, stored)


def inverse_of_pair(a):
    step = 8
    lane = lanes_of((step, WIDE))
    sub = lax.broadcasted_iota(jnp.int32, (step, WIDE), 0)
    base = jnp.where(lane < HALF, 0, HALF)
    rows = [a[i * step : (i + 1) * step] for i in range(HALF // step)]

    def spread(x, m):
        return jnp.broadcast_to(x[m : m + 1], (step, WIDE))

    for block in range(HALF // step):
        first = block * step
        columns = [
            [jnp.take_along_axis(r, base + (first + j), axis=1) for j in range(step)] for r in rows
        ]
        inside = (lane - base >= first) & (lane - base < first + step)
        identity = jnp.where(lane - base == first + sub, 1.0, 0.0)
        panel = jnp.where(inside, identity, rows[block])
        diag = list(columns[block])
        for m in range(step):
            inverse = 1.0 / spread(diag[m], m)
            is_row = sub == m
            keep = jnp.where(is_row, 0.0, diag[m])
            for j in range(m + 1, step):
                over = spread(diag[j], m)
                diag[j] = jnp.where(is_row, 0.0, diag[j]) + jnp.where(is_row, over, -(keep * over)) * inverse
            over = spread(panel, m)
            panel = jnp.where(is_row, 0.0, panel) + jnp.where(is_row, over, -(keep * over)) * inverse
        spreads = [spread(panel, j) for j in range(step)]
        for i in range(HALF // step):
            if i == block:
                rows[i] = panel
                continue
            taken = [c * p for c, p in zip(columns[i], spreads)]
            while len(taken) > 1:
                taken = [x + y for x, y in zip(taken[::2], taken[1::2])]
            rows[i] = jnp.where(inside, 0.0, rows[i]) - taken[0]
    return jnp.concatenate(rows, axis=0)


def score_kernel(core_ref, got_ref, own, over, out_ref, rolled):
    parts = got_ref.shape[0] // 2
    part = HALF // parts
    blocks = 2 * (got_ref.shape[1] // part - 1)
    lane = lanes_of((HALF, WIDE))
    row = lax.broadcasted_iota(jnp.int32, (HALF, WIDE), 0)
    left = lane < HALF
    at = got_ref.shape[1] - part
    moments = jnp.concatenate([got_ref[2 * y, at:] + got_ref[2 * y + 1, at:] for y in range(parts)], axis=0)
    count = jnp.broadcast_to(moments[0:1, 1:2], (HALF, WIDE))
    moments = jnp.where((row == 0) & (lane == 1), jnp.broadcast_to(moments[1:2, 0:1], (HALF, WIDE)), moments)
    mean = moments / count
    diagonal = jnp.where((lane == row) | (lane == row + HALF), mean, 0.0)
    trace_in = jnp.sum(jnp.where(left, diagonal, 0.0))
    trace_out = jnp.sum(jnp.where(left, 0.0, diagonal))
    extra = jnp.where(left, trace_in, trace_out) * (damping / HALF)
    damped = mean + jnp.where((lane == row) | (lane == row + HALF), extra, 0.0)
    factors = inverse_of_pair(damped)
    top = jnp.where(left, factors, 0.0)
    right = jnp.concatenate([top, pltpu.roll(top, HALF, 1)], axis=0)
    empty = jnp.zeros_like(right)
    right = in_two(
        jnp.concatenate(
            [jnp.concatenate([right, empty], axis=1), jnp.concatenate([empty, right], axis=1)], axis=0
        )
    )
    outer = in_two(factors[:, HALF:])
    half_lane = lanes_of((HALF // 2, WIDE)) < HALF

    def block_of(i):
        z, x, core = i // 4, i // 2 % 2, i % 2
        at = (2 * z + core) * part
        return [got_ref[2 * y + x, at : at + part] for y in range(parts)]

    group = 16
    apart = HALF // 2 + 1
    for b in range(0, blocks, group):
        g = [
            jnp.concatenate(block_of(i), axis=0)
            for i in range(b, b + group)
        ]
        g = jnp.concatenate([jnp.concatenate(g[i : i + 2], axis=1) for i in range(0, group, 2)], axis=0)
        inner = three_pass(in_two(g), right, NN)
        inner = jnp.concatenate([inner[HALF * i : HALF * (i + 1)] for i in range(group // 2)], axis=1)
        done = three_pass(outer, in_two(inner), NN)
        for i in range(group):
            up = done[: HALF // 2, WIDE * i : WIDE * (i + 1)]
            low = done[HALF // 2 :, WIDE * i : WIDE * (i + 1)]
            at = 2 * (b + i)
            rolled[pl.ds(at * apart, HALF // 2)] = jnp.where(half_lane, up, pltpu.roll(low, HALF, 1))
            rolled[pl.ds((at + 1) * apart, HALF // 2)] = jnp.where(half_lane, pltpu.roll(up, HALF, 1), low)
    scores = jnp.zeros((2 * blocks, 2 * HALF), f32)
    deep = 8
    for k in range(0, HALF // 2, deep):
        first = jnp.concatenate([rolled[pl.ds(k + i, 2 * blocks, apart)] for i in range(deep)], axis=1)
        second = jnp.concatenate([jnp.concatenate([own[k + i], over[k + i]], axis=0) for i in range(deep)], axis=1)
        scores += three_pass(in_two(first), in_two(second), NT)
    scores *= 1.0 / math.sqrt(2 * HALF * HALF)
    out_ref[...] = jnp.where(core_ref[0] == 0, scores, pltpu.roll(scores, HALF, 1))


def score(place, got, own, over):
    blocks = 2 * (got.shape[1] // (2 * HALF // got.shape[0]) - 1)
    vmem = pl.BlockSpec(memory_space=pltpu.VMEM)
    return pl.pallas_call(
        score_kernel,
        in_specs=[pl.BlockSpec(memory_space=pltpu.SMEM)] + [vmem] * 3,
        out_specs=vmem,
        out_shape=jax.ShapeDtypeStruct((2 * blocks, WIDE), f32),
        scratch_shapes=[
            pltpu.VMEM((2 * blocks * (HALF // 2 + 1), WIDE), f32),
        ],
        compiler_params=pltpu.CompilerParams(vmem_limit_bytes=16 * 2**20),
        cost_estimate=cost(200_000_000, 6 * 2**20),
        name="score",
    )(place, got, own, over)


def shards(activations, out_grads, lengths, input_proj, output_proj, stored_proj):
    seq_count = lax.axis_size(SEQ)
    core = lax.axis_index("core")
    seq_dev = activations.shape[2]
    start = (lax.axis_index(SEQ) * seq_dev).astype(jnp.int32).reshape(1)
    place = core.astype(jnp.int32).reshape(1)
    terms = project(lengths, start, place, activations, out_grads, input_proj, output_proj, seq_count)
    part = terms.shape[2] // 2
    terms = terms.reshape(-1, 2 * part, WIDE)
    arrived = lax.all_to_all(terms, SEQ + ("core",), 0, 0, tiled=True)
    seq_sum = arrived.reshape(seq_count, 2, 2 * part, WIDE).sum(axis=0)
    moments = seq_sum[:, part:].sum(axis=0)
    rows = jnp.concatenate([seq_sum[:, :part].reshape(-1, WIDE), moments], axis=0)
    z_count = lax.axis_size("z")
    z_all = lax.all_to_all(jnp.broadcast_to(rows, (z_count, *rows.shape)), "z", 0, 0, tiled=True)
    moments = z_all[:, 2 * part :].sum(axis=0)
    rows = jnp.concatenate([z_all[:, : 2 * part].reshape(-1, WIDE), moments], axis=0)
    rest = SEQ + ("x_hi",)
    got = lax.all_to_all(jnp.broadcast_to(rows, (lax.axis_size(rest), *rows.shape)), rest, 0, 0, tiled=True)
    own, send = pack(place, stored_proj)
    over = lax.ppermute(send, "core", [(0, 1), (1, 0)])
    partial = score(place, got, own, over)
    back = lax.all_to_all(partial.reshape(-1, 2, WIDE), BLK, 0, 0, tiled=True)
    back = back.reshape(-1, 2, 2, WIDE).sum(axis=1)
    return jnp.swapaxes(back, 0, 1).reshape(2, -1)


def solution(mesh):
    seq, blk = mesh.shape["seq"], mesh.shape["blk"]
    fine = Mesh(mesh.devices.reshape(seq // 2, 2, blk // 4, 2, 2), SEQ + BLK)
    return jax.shard_map(
        shards,
        mesh=fine,
        in_specs=(
            P(None, BLK, SEQ, None),
            P(None, BLK, SEQ, None),
            P(BLK),
            P(),
            P(),
            P(SEQ + BLK, None, None, None),
        ),
        out_specs=P(BLK, SEQ),
        check_vma=False,
    )
```

```python
import functools
import math

import jax
import jax.numpy as jnp
from jax import lax
from jax.experimental import pallas as pl
from jax.experimental.pallas import tpu as pltpu
from jax.sharding import Mesh, PartitionSpec as P


damping = 0.1
SEQ = ("y", "x_lo")
BLK = ("z", "x_hi", "core")
HALF = 64
WIDE = 128
f32 = jnp.float32
bf16 = jnp.bfloat16
NT = (((1,), (1,)), ((), ()))
NN = (((1,), (0,)), ((), ()))


def cost(flops, moved):
    return pl.CostEstimate(flops=flops, bytes_accessed=moved, transcendentals=0)


def lanes_of(shape):
    return lax.broadcasted_iota(jnp.int32, shape, len(shape) - 1)


def in_two(x):
    high = x.astype(bf16)
    return high, (x - high.astype(f32)).astype(bf16)


def three_pass(a, b, dims):
    dot = functools.partial(lax.dot_general, dimension_numbers=dims, preferred_element_type=f32)
    rows = a[0].shape[0]
    stacked = dot(jnp.concatenate(a, axis=0), b[0])
    return stacked[:rows] + (stacked[rows:] + dot(a[0], b[1]))


def project_kernel(length_ref, start_ref, place_ref, act_hbm, grad_hbm, win_hbm, wout_hbm, out_ref, act, grad, win, wout, sems):
    layers, rolls, seq, width = act.shape
    cuts = sems.shape[2]
    depth = width // cuts
    sides = ((act_hbm, act, win_hbm, win), (grad_hbm, grad, wout_hbm, wout))

    def copies(l, side, k):
        big_from, big_to, weight_from, weight_to = sides[side]
        span = pl.ds(k * depth, depth)
        return (
            pltpu.make_async_copy(weight_from.at[l, :, span], weight_to.at[l, :, span], sems.at[l, side, k, 0]),
            pltpu.make_async_copy(
                big_from.at[l, :, :, span], big_to.at[l, :, :, span], sems.at[l, side, k, 1]
            ),
        )

    every = [(l, side, k) for l in range(layers) for k in range(cuts) for side in range(2)]
    for place in every:
        for copy in copies(*place):
            copy.start()
    dot = functools.partial(lax.dot_general, dimension_numbers=NT, preferred_element_type=f32)
    lane = lanes_of((HALF, WIDE))
    row = lax.broadcasted_iota(jnp.int32, (HALF, WIDE), 0)
    position = lax.broadcasted_iota(jnp.int32, (seq, WIDE), 0)
    part = HALF // out_ref.shape[0]
    for l in range(layers):
        halves = [None, None]
        for k in range(cuts):
            for side in range(2):
                for copy in copies(l, side, k):
                    copy.wait()
            span = slice(k * depth, (k + 1) * depth)
            for side in range(2):
                _, big, _, weight = sides[side]
                term = jnp.concatenate([dot(big[l, r, :, span], weight[l, :, span]) for r in range(rolls)], axis=0)
                halves[side] = term if k == 0 else halves[side] + term
        both = jnp.concatenate(halves, axis=1)
        grams = []
        count = jnp.int32(0)
        for r in range(rolls):
            live = length_ref[r] - start_ref[0]
            c = both[r * seq : (r + 1) * seq] * (position < live).astype(f32)
            grams.append(three_pass(in_two(c.T), in_two(c), NN))
            count += jnp.clip(live, 0, seq)
        pair = jnp.where(lane < HALF, grams[0][HALF:], pltpu.roll(grams[1][HALF:], HALF, 1))
        total = grams[0] + grams[1]
        moments = jnp.where(lane < HALF, total[:HALF], total[HALF:])
        moments = jnp.where((row == 0) & (lane == 1), count.astype(f32), moments)
        for y in range(out_ref.shape[0]):
            out_ref[y, l, 0:part] = pair[y * part : (y + 1) * part]
            out_ref[y, l, part : 2 * part] = moments[y * part : (y + 1) * part]


def project(lengths, start, place, activations, out_grads, input_proj, output_proj, parts):
    layers, rolls, seq, width = activations.shape
    rank = input_proj.shape[1]
    cuts = 4
    part = HALF // parts
    anywhere = pl.BlockSpec(memory_space=pl.ANY)
    return pl.pallas_call(
        project_kernel,
        in_specs=[pl.BlockSpec(memory_space=pltpu.SMEM)] * 3 + [anywhere] * 4,
        out_specs=pl.BlockSpec(memory_space=pltpu.VMEM),
        out_shape=jax.ShapeDtypeStruct((parts, layers, 2 * part, WIDE), f32),
        scratch_shapes=[
            pltpu.VMEM(activations.shape, activations.dtype),
            pltpu.VMEM(out_grads.shape, out_grads.dtype),
            pltpu.VMEM(input_proj.shape, input_proj.dtype),
            pltpu.VMEM(output_proj.shape, output_proj.dtype),
            pltpu.SemaphoreType.DMA((layers, 2, cuts, 2)),
        ],
        compiler_params=pltpu.CompilerParams(vmem_limit_bytes=65_700_000),
        cost_estimate=cost(4 * layers * rolls * seq * width * rank, 4 * layers * rolls * seq * width),
        name="project",
    )(lengths, start, place, activations, out_grads, input_proj, output_proj)


def pack_kernel(layer_ref, keep_top, keep_low, send_top, send_low, keep_ref, send_ref):
    for k in range(keep_ref.shape[0]):
        keep_ref[k] = jnp.concatenate([keep_top[:, 0, k, :], keep_low[:, 0, k, :]], axis=1)
        send_ref[k] = jnp.concatenate([send_top[:, 0, k, :], send_low[:, 0, k, :]], axis=1)


def pack(layer, stored):
    train, _, rank, _ = stored.shape
    chunk = 8
    steps = rank // 2 // chunk

    def spec(other, low):
        def at(i, layer):
            l = 1 - layer[0] if other else layer[0]
            return (0, l, i + (steps if low else 0), 0)

        return pl.BlockSpec((train, 1, chunk, rank), at)

    out = pl.BlockSpec((chunk, train, WIDE), lambda i, layer: (i, 0, 0))
    shape = jax.ShapeDtypeStruct((rank // 2, train, WIDE), f32)
    return pl.pallas_call(
        pack_kernel,
        grid_spec=pltpu.PrefetchScalarGridSpec(
            num_scalar_prefetch=1,
            grid=(steps,),
            in_specs=[spec(False, False), spec(False, True), spec(True, False), spec(True, True)],
            out_specs=[out, out],
        ),
        out_shape=[shape, shape],
        compiler_params=pltpu.CompilerParams(vmem_limit_bytes=12 * 2**20),
        cost_estimate=cost(10_000_000, 6 * 2**20),
        name="pack",
    )(layer, stored, stored, stored, stored)


def inverse_of_pair(a):
    step = 8
    lane = lanes_of((step, WIDE))
    sub = lax.broadcasted_iota(jnp.int32, (step, WIDE), 0)
    base = jnp.where(lane < HALF, 0, HALF)
    rows = [a[i * step : (i + 1) * step] for i in range(HALF // step)]

    def spread(x, m):
        return jnp.broadcast_to(x[m : m + 1], (step, WIDE))

    for block in range(HALF // step):
        first = block * step
        columns = [
            [jnp.take_along_axis(r, base + (first + j), axis=1) for j in range(step)] for r in rows
        ]
        inside = (lane - base >= first) & (lane - base < first + step)
        identity = jnp.where(lane - base == first + sub, 1.0, 0.0)
        panel = jnp.where(inside, identity, rows[block])
        diag = list(columns[block])
        for m in range(step):
            inverse = 1.0 / spread(diag[m], m)
            is_row = sub == m
            keep = jnp.where(is_row, 0.0, diag[m])
            for j in range(m + 1, step):
                over = spread(diag[j], m)
                diag[j] = jnp.where(is_row, 0.0, diag[j]) + jnp.where(is_row, over, -(keep * over)) * inverse
            over = spread(panel, m)
            panel = jnp.where(is_row, 0.0, panel) + jnp.where(is_row, over, -(keep * over)) * inverse
        spreads = [spread(panel, j) for j in range(step)]
        for i in range(HALF // step):
            if i == block:
                rows[i] = panel
                continue
            taken = [c * p for c, p in zip(columns[i], spreads)]
            while len(taken) > 1:
                taken = [x + y for x, y in zip(taken[::2], taken[1::2])]
            rows[i] = jnp.where(inside, 0.0, rows[i]) - taken[0]
    return jnp.concatenate(rows, axis=0)


def score_kernel(core_ref, got_ref, own, over, out_ref, rolled):
    parts = got_ref.shape[0] // 2
    part = HALF // parts
    blocks = 2 * (got_ref.shape[1] // part - 1)
    lane = lanes_of((HALF, WIDE))
    row = lax.broadcasted_iota(jnp.int32, (HALF, WIDE), 0)
    left = lane < HALF
    at = got_ref.shape[1] - part
    moments = jnp.concatenate([got_ref[2 * y, at:] + got_ref[2 * y + 1, at:] for y in range(parts)], axis=0)
    count = jnp.broadcast_to(moments[0:1, 1:2], (HALF, WIDE))
    moments = jnp.where((row == 0) & (lane == 1), jnp.broadcast_to(moments[1:2, 0:1], (HALF, WIDE)), moments)
    mean = moments / count
    diagonal = jnp.where((lane == row) | (lane == row + HALF), mean, 0.0)
    trace_in = jnp.sum(jnp.where(left, diagonal, 0.0))
    trace_out = jnp.sum(jnp.where(left, 0.0, diagonal))
    extra = jnp.where(left, trace_in, trace_out) * (damping / HALF)
    damped = mean + jnp.where((lane == row) | (lane == row + HALF), extra, 0.0)
    factors = inverse_of_pair(damped)
    top = jnp.where(left, factors, 0.0)
    right = jnp.concatenate([top, pltpu.roll(top, HALF, 1)], axis=0)
    empty = jnp.zeros_like(right)
    right = in_two(
        jnp.concatenate(
            [jnp.concatenate([right, empty], axis=1), jnp.concatenate([empty, right], axis=1)], axis=0
        )
    )
    outer = in_two(factors[:, HALF:])
    half_lane = lanes_of((HALF // 2, WIDE)) < HALF

    def block_of(i):
        z, x, core = i // 4, i // 2 % 2, i % 2
        at = (2 * z + core) * part
        return [got_ref[2 * y + x, at : at + part] for y in range(parts)]

    group = 16
    apart = HALF // 2 + 1
    for b in range(0, blocks, group):
        g = [
            jnp.concatenate(block_of(i), axis=0)
            for i in range(b, b + group)
        ]
        g = jnp.concatenate([jnp.concatenate(g[i : i + 2], axis=1) for i in range(0, group, 2)], axis=0)
        inner = three_pass(in_two(g), right, NN)
        inner = jnp.concatenate([inner[HALF * i : HALF * (i + 1)] for i in range(group // 2)], axis=1)
        done = three_pass(outer, in_two(inner), NN)
        for i in range(group):
            up = done[: HALF // 2, WIDE * i : WIDE * (i + 1)]
            low = done[HALF // 2 :, WIDE * i : WIDE * (i + 1)]
            at = 2 * (b + i)
            rolled[pl.ds(at * apart, HALF // 2)] = jnp.where(half_lane, up, pltpu.roll(low, HALF, 1))
            rolled[pl.ds((at + 1) * apart, HALF // 2)] = jnp.where(half_lane, pltpu.roll(up, HALF, 1), low)
    scores = jnp.zeros((2 * blocks, 2 * HALF), f32)
    deep = 16
    for k in range(0, HALF // 2, deep):
        first = jnp.concatenate([rolled[pl.ds(k + i, 2 * blocks, apart)] for i in range(deep)], axis=1)
        second = jnp.concatenate([jnp.concatenate([own[k + i], over[k + i]], axis=0) for i in range(deep)], axis=1)
        scores += three_pass(in_two(first), in_two(second), NT)
    scores *= 1.0 / math.sqrt(2 * HALF * HALF)
    out_ref[...] = jnp.where(core_ref[0] == 0, scores, pltpu.roll(scores, HALF, 1))


def score(place, got, own, over):
    blocks = 2 * (got.shape[1] // (2 * HALF // got.shape[0]) - 1)
    vmem = pl.BlockSpec(memory_space=pltpu.VMEM)
    return pl.pallas_call(
        score_kernel,
        in_specs=[pl.BlockSpec(memory_space=pltpu.SMEM)] + [vmem] * 3,
        out_specs=vmem,
        out_shape=jax.ShapeDtypeStruct((2 * blocks, WIDE), f32),
        scratch_shapes=[
            pltpu.VMEM((2 * blocks * (HALF // 2 + 1), WIDE), f32),
        ],
        compiler_params=pltpu.CompilerParams(vmem_limit_bytes=16 * 2**20),
        cost_estimate=cost(200_000_000, 6 * 2**20),
        name="score",
    )(place, got, own, over)


def shards(activations, out_grads, lengths, input_proj, output_proj, stored_proj):
    seq_count = lax.axis_size(SEQ)
    core = lax.axis_index("core")
    seq_dev = activations.shape[2]
    start = (lax.axis_index(SEQ) * seq_dev).astype(jnp.int32).reshape(1)
    place = core.astype(jnp.int32).reshape(1)
    terms = project(lengths, start, place, activations, out_grads, input_proj, output_proj, seq_count)
    part = terms.shape[2] // 2
    terms = terms.reshape(-1, 2 * part, WIDE)
    arrived = lax.all_to_all(terms, SEQ + ("core",), 0, 0, tiled=True)
    seq_sum = arrived.reshape(seq_count, 2, 2 * part, WIDE).sum(axis=0)
    moments = seq_sum[:, part:].sum(axis=0)
    rows = jnp.concatenate([seq_sum[:, :part].reshape(-1, WIDE), moments], axis=0)
    z_count = lax.axis_size("z")
    z_all = lax.all_to_all(jnp.broadcast_to(rows, (z_count, *rows.shape)), "z", 0, 0, tiled=True)
    moments = z_all[:, 2 * part :].sum(axis=0)
    rows = jnp.concatenate([z_all[:, : 2 * part].reshape(-1, WIDE), moments], axis=0)
    rest = SEQ + ("x_hi",)
    got = lax.all_to_all(jnp.broadcast_to(rows, (lax.axis_size(rest), *rows.shape)), rest, 0, 0, tiled=True)
    own, send = pack(place, stored_proj)
    over = lax.ppermute(send, "core", [(0, 1), (1, 0)])
    partial = score(place, got, own, over)
    back = lax.all_to_all(partial.reshape(-1, 2, WIDE), BLK, 0, 0, tiled=True)
    back = back.reshape(-1, 2, 2, WIDE).sum(axis=1)
    return jnp.swapaxes(back, 0, 1).reshape(2, -1)


def solution(mesh):
    seq, blk = mesh.shape["seq"], mesh.shape["blk"]
    fine = Mesh(mesh.devices.reshape(seq // 2, 2, blk // 4, 2, 2), SEQ + BLK)
    return jax.shard_map(
        shards,
        mesh=fine,
        in_specs=(
            P(None, BLK, SEQ, None),
            P(None, BLK, SEQ, None),
            P(BLK),
            P(),
            P(),
            P(SEQ + BLK, None, None, None),
        ),
        out_specs=P(BLK, SEQ),
        check_vma=False,
    )
```
